32 devices in a mesh: ep: 8 (over z, x), tp: 4 (over y, core).
Axes of the slice: x: 2, y: 2, z: 4, core: 2. Of those that a mesh axis runs over, the one named last changes fastest.
Arguments:
- hidden: bfloat16 [512, 2880], P('ep'), may hold values from -0.59765625 to 0.59765625
- queries: bfloat16 [512, 2048], P('ep', 'tp'), may hold values from -160 to 160
- new_keys: bfloat16 [512, 256], P('ep', 'tp'), may hold values from -6 to 6
- new_values: bfloat16 [512, 256], P('ep', 'tp'), may hold values from -6 to 6
- key_cache: bfloat16 [64, 4, 64, 1024], P('ep', 'tp'), may hold values from -6 to 6
- value_cache: bfloat16 [64, 4, 64, 1024], P('ep', 'tp'), may hold values from -6 to 6
- cache_lengths: int32 [64], P('ep'), may hold values from 16 to 1024
- w_out: bfloat16 [2048, 2880], P('tp'), may hold values from -0.125 to 0.125
- w_router: bfloat16 [2880, 8], replicated, may hold values from -0.109375 to 0.109375
- routes: int32 [512, 4], P('ep'), may hold values from 0 to 7, all different within a row; in each aligned block of 16 rows (0 to 15, 16 to 31, ...) at most 16 rows name the same one
- w_gate: bfloat16 [8, 2880, 1536], P('ep', None, 'tp'), may hold values from -0.109375 to 0.109375
- w_up: bfloat16 [8, 2880, 1536], P('ep', None, 'tp'), may hold values from -0.109375 to 0.109375
- w_down: bfloat16 [8, 1536, 2880], P('ep', 'tp'), may hold values from -0.15625 to 0.15625
Outputs:
- layer_out: bfloat16 [512, 2880], P(('ep', 'tp'))
The draws below stay inside these ranges and needn't reach their ends.
Inputs may be any that keep to these rules, and one draw needn't show every extreme that they name: `routes`: each token names 4 different experts; in each aligned block of 16 tokens no expert is named by more than 16 tokens, and in some blocks one expert is named by exactly 16.
All inputs are finite; a program needn't handle non-finite values.
Results may differ from the reference program's by a relative error of at most 0.02.
Values may be sent and summed in bfloat16 or wider, within the bound.
No kernel may reach another device: no remote copies, remote signals or barrier semaphores. Data moves between devices by JAX's collectives and lax.ppermute only.
A program may use at most 64 MiB of HBM per device.

```python
import math
import jax
import jax.numpy as jnp
import numpy as np
from jax import lax

D = 2880
HEADS = 32
KV_HEADS = 4
HEAD_DIM = 64
FF = 1536
TOP = 4
SEQ_DEV = 8
LEN = 1024
EXPERTS = 8
SEQS = 64
TOKENS = 512
TOK_EP = 64
BLOCK = 16
CAP = 16
N_EP = 8
N_TP = 4


def draw_queries(key, part):
    shape_q = (TOKENS, HEADS * HEAD_DIM)
    values = jnp.clip(jax.random.normal(jax.random.fold_in(key, 1), shape_q, jnp.float32), -6.0, 6.0)
    return values.astype(jnp.bfloat16)


def draw_key_cache(key, part):
    base_draw = jax.random.normal(jax.random.fold_in(key, 3), (SEQS, KV_HEADS, HEAD_DIM, LEN), jnp.float32)
    base_draw = jnp.clip(base_draw, -6.0, 6.0)
    return base_draw.astype(jnp.bfloat16)


def place_ends(array, stream_key, low, high):
    dims = array.shape
    index_at = [jax.random.randint(jax.random.fold_in(stream_key, axis), (), 0, dims[axis]) for axis in range(len(dims))]
    array = array.at[tuple(index_at)].set(low)
    longest = dims.index(max(dims))
    index_at[longest] = (index_at[longest] + 1) % dims[longest]
    return array.at[tuple(index_at)].set(high)


def levels(key, dims, cuts, low, largest):
    gain = 1.0
    for axis_at, parts in cuts:
        steps = jax.random.uniform(jax.random.fold_in(jax.random.fold_in(key, 6), axis_at), (parts,), jnp.float32, low / len(cuts), largest / len(cuts))
        gain = gain * jnp.repeat(jnp.exp(steps), dims[axis_at] // parts).reshape((-1,) + (1,) * (len(dims) - 1 - axis_at))
    return gain


def deal_out(stream_key, own, number, rows, amount, top, reach, lean):
    ranking = jax.random.permutation(stream_key, amount)
    packed, common = portions_of(amount, rows * top, reach, lean, True), portions_of(amount, rows * top, reach, lean, False)
    places = jnp.arange(amount)

    def named(lengths, turn):
        used = int((lengths > 0).sum())
        fixed = max(1, used // 4)
        passed = fixed + (places - fixed + turn * (used - fixed)) % max(1, amount - fixed)
        return jnp.zeros((amount,), jnp.int32).at[ranking[jnp.where(places < fixed, places, passed)]].set(jnp.asarray(lengths, jnp.int32))

    lengths = jnp.where(number % 4 == 0, named(packed, number // 4), named(common, number - number // 4 - 1))
    mixed = jax.random.permutation(jax.random.fold_in(own, 3), amount)
    giver, receiver = mixed[0:amount // 2 * 2:2], mixed[1:amount // 2 * 2:2]
    slack = jnp.minimum(lengths[giver] - 1, reach - lengths[receiver]) // 2
    slack = jnp.where((giver == ranking[0]) | (receiver == ranking[0]) | (lengths[receiver] == 0), 0, jnp.maximum(slack, 0))
    passed = jax.random.randint(jax.random.fold_in(own, 4), (amount // 2,), 0, 1 << 20) % (slack + 1)
    lengths = lengths.at[giver].add(-passed).at[receiver].add(passed)
    items = jnp.searchsorted(jnp.cumsum(lengths), jnp.arange(rows * top), side="right").astype(jnp.int32)
    table = items.reshape(top, rows).T
    table = table[jax.random.permutation(jax.random.fold_in(own, 1), rows)]
    turn = jax.random.randint(jax.random.fold_in(own, 2), (rows, 1), 0, top)
    return jnp.take_along_axis(table, (jnp.arange(top)[None, :] + turn) % top, axis=1)


def portions_of(count, total, most, slope, full):
    weights = [(1 << 20) // math.isqrt(standing ** slope) + 1 for standing in range(1, count + 1)]
    largest = most if full else min(most, max(-(-total // count), total * weights[0] // sum(weights)))
    least = 1 if total - largest >= count - 1 else 0
    holding, rest = [largest] + [least] * (count - 1), total - largest - least * (count - 1)
    while rest > 0:
        movable = [i for i in range(1, count) if holding[i] < largest] or [i for i in range(1, count) if holding[i] < most]
        mass, left = sum([weights[i] for i in movable]), rest
        for i in movable:
            extra = min(most - holding[i], max(1, left * weights[i] // mass), rest)
            holding[i] = holding[i] + extra
            rest = rest - extra
    return np.array(holding)


def centred(key, dims, width, limit, split=(), kind=jnp.bfloat16):
    values = jax.random.normal(key, dims, jnp.float32) * width
    if len(split) > 0:
        values = levels(key, dims, split, -0.22, 0.18) * values
    return jnp.clip(values, min=-limit, max=limit).astype(kind)


def setup_inputs(seed: int = 0) -> dict:
    keys = jax.random.split(jax.random.key(seed), 14)
    hidden = centred(keys[0], (TOKENS, D), 0.1, 0.59765625, ((0, 8),))
    queries = draw_queries(jax.random.fold_in(keys[13], 71), 0)
    new_keys = centred(keys[2], (TOKENS, KV_HEADS * HEAD_DIM), 1.0, 6.0, ((0, 8), (1, 4)))
    new_values = centred(keys[3], (TOKENS, KV_HEADS * HEAD_DIM), 1.0, 6.0, ((0, 8), (1, 4)))
    key_cache = draw_key_cache(jax.random.fold_in(keys[13], 71), 0)
    value_cache = centred(keys[5], (SEQS, KV_HEADS, HEAD_DIM, LEN), 1.0, 6.0, ((0, 8), (1, 4)))
    cache_lengths = place_ends(jax.random.randint(keys[6], (SEQS,), 16, LEN + 1), jax.random.fold_in(keys[6], 1), 16, LEN).astype(jnp.int32)
    w_out = centred(keys[7], (HEADS * HEAD_DIM, D), (HEADS * HEAD_DIM) ** -0.5, 0.125, ((0, 4),))
    w_router = centred(keys[8], (D, EXPERTS), D ** -0.5, 0.109375)
    routes_keys = jax.random.split(jax.random.fold_in(keys[9], 1), TOKENS // BLOCK)
    routes_turns = jax.random.permutation(jax.random.fold_in(keys[9], 3), TOKENS // BLOCK)
    routes = jax.vmap(lambda own, number: deal_out(jax.random.fold_in(keys[9], 2), own, number, BLOCK, EXPERTS, TOP, CAP, 2))(routes_keys, routes_turns).reshape((TOKENS, TOP))
    w_gate = centred(keys[10], (EXPERTS, D, FF), D ** -0.5, 0.109375, ((0, 8), (2, 4)))
    w_up = centred(keys[11], (EXPERTS, D, FF), D ** -0.5, 0.109375, ((0, 8), (2, 4)))
    w_down = centred(keys[12], (EXPERTS, FF, D), FF ** -0.5, 0.15625, ((0, 8), (1, 4)))
    return dict(hidden=hidden, queries=queries, new_keys=new_keys, new_values=new_values, key_cache=key_cache, value_cache=value_cache, cache_lengths=cache_lengths, w_out=w_out, w_router=w_router, routes=routes, w_gate=w_gate, w_up=w_up, w_down=w_down)


def attend_block(queries, new_keys, new_values, key_cache, value_cache, cache_lengths):
    seq_count, kv_count, head_dim, length = key_cache.shape
    new_count = queries.shape[0] // seq_count
    group_size = queries.shape[1] // (kv_count * head_dim)
    row_count = new_count * group_size
    scale = head_dim ** (-0.5)
    query_block = queries.astype(jnp.float32).reshape(seq_count, new_count, kv_count, group_size, head_dim)
    query_block = query_block.transpose(0, 2, 1, 3, 4).reshape(seq_count, kv_count, row_count, head_dim)
    fresh_keys = new_keys.astype(jnp.float32).reshape(seq_count, new_count, kv_count, head_dim).transpose(0, 2, 1, 3)
    fresh_values = new_values.astype(jnp.float32).reshape(seq_count, new_count, kv_count, head_dim).transpose(0, 2, 1, 3)
    cache_scores = jnp.einsum('skrd,skdl->skrl', query_block, key_cache.astype(jnp.float32)) * scale
    in_cache = jnp.arange(length)[None, :] < cache_lengths[:, None]
    cache_scores = jnp.where(in_cache[:, None, None, :], cache_scores, -1e+30)
    fresh_scores = jnp.einsum('skrd,sknd->skrn', query_block, fresh_keys) * scale
    causal = (jnp.arange(row_count) // group_size)[:, None] >= jnp.arange(new_count)[None, :]
    fresh_scores = jnp.where(causal[None, None, :, :], fresh_scores, -1e+30)
    row_max = jnp.maximum(lax.optimization_barrier(jnp.max(cache_scores, -1, keepdims=True)), lax.optimization_barrier(jnp.max(fresh_scores, -1, keepdims=True)))
    cache_exp = jnp.exp(cache_scores - row_max)
    fresh_exp = jnp.exp(fresh_scores - row_max)
    denom_sum = lax.optimization_barrier(jnp.sum(cache_exp, -1, keepdims=True)) + lax.optimization_barrier(jnp.sum(fresh_exp, -1, keepdims=True))
    cache_probs = (cache_exp / denom_sum).astype(jnp.bfloat16).astype(jnp.float32)
    fresh_probs = (fresh_exp / denom_sum).astype(jnp.bfloat16).astype(jnp.float32)
    head_mix = jnp.einsum('skrl,skdl->skrd', cache_probs, value_cache.astype(jnp.float32))
    head_mix = head_mix + jnp.einsum('skrn,sknd->skrd', fresh_probs, fresh_values)
    head_mix = head_mix.reshape(seq_count, kv_count, new_count, group_size, head_dim).transpose(0, 2, 1, 3, 4)
    return head_mix.reshape(seq_count * new_count, kv_count * group_size * head_dim).astype(jnp.bfloat16)

def expert_rows(pieces):
    buffer_rows, gate_weight, up_weight, down_weight = pieces
    gate_proj = jnp.dot(buffer_rows, gate_weight, preferred_element_type=jnp.float32)
    up_proj = jnp.dot(buffer_rows, up_weight, preferred_element_type=jnp.float32)
    activated = ((up_proj + 1.0) * gate_proj * jax.nn.sigmoid(1.702 * gate_proj)).astype(jnp.bfloat16)
    return jnp.dot(activated, down_weight, preferred_element_type=jnp.float32)

def reference(hidden, queries, new_keys, new_values, key_cache, value_cache, cache_lengths, w_out, w_router, routes, w_gate, w_up, w_down):
    blocks = (queries.reshape(N_EP, TOK_EP, HEADS * HEAD_DIM), new_keys.reshape(N_EP, TOK_EP, KV_HEADS * HEAD_DIM), new_values.reshape(N_EP, TOK_EP, KV_HEADS * HEAD_DIM), key_cache.reshape(N_EP, SEQ_DEV, KV_HEADS, HEAD_DIM, LEN), value_cache.reshape(N_EP, SEQ_DEV, KV_HEADS, HEAD_DIM, LEN), cache_lengths.reshape(N_EP, SEQ_DEV))
    attended = lax.map(lambda pieces: attend_block(*pieces), blocks).reshape(TOKENS, HEADS * HEAD_DIM)
    residual = hidden.astype(jnp.float32) + jnp.dot(attended, w_out, preferred_element_type=jnp.float32)
    normed = (residual * lax.rsqrt(lax.optimization_barrier(jnp.mean(residual * residual, -1, keepdims=True)) + 1e-05)).astype(jnp.bfloat16)
    logits = jnp.dot(normed, w_router, preferred_element_type=jnp.float32)
    picked = jnp.take_along_axis(logits, routes, 1)
    picked_exp = jnp.exp(picked)
    weights = picked_exp / lax.optimization_barrier(jnp.sum(picked_exp, -1, keepdims=True))
    flat_routes = routes.reshape(-1).astype(jnp.int32)
    one_hot = (flat_routes[:, None] == jnp.arange(EXPERTS, dtype=jnp.int32)[None, :]).astype(jnp.int32)
    slot_rank = lax.optimization_barrier(jnp.sum((jnp.cumsum(one_hot, 0) - one_hot) * one_hot, 1)).astype(jnp.int32)
    capacity = N_EP * N_TP * CAP
    buffer = jnp.zeros((EXPERTS, capacity, D), jnp.bfloat16)
    buffer = buffer.at[flat_routes, slot_rank].set(jnp.repeat(normed, TOP, axis=0))
    outputs = lax.map(expert_rows, (buffer, w_gate, w_up, w_down))
    routed = outputs[flat_routes, slot_rank].reshape(TOKENS, TOP, D)
    mixture = lax.optimization_barrier(jnp.sum(weights[:, :, None] * routed, 1))
    return (residual + mixture).astype(jnp.bfloat16)
```

```python
import jax
import jax.numpy as jnp
from jax import lax
from jax.sharding import PartitionSpec as P


def attend(queries, new_keys, new_values, key_cache, value_cache, cache_lengths):
    seq_count, kv_count, head_dim, length = key_cache.shape
    new_count = queries.shape[0] // seq_count
    group_size = queries.shape[1] // (kv_count * head_dim)
    row_count = new_count * group_size
    scale = head_dim ** (-0.5)
    query_block = queries.reshape(seq_count, new_count, kv_count, group_size, head_dim)
    query_block = query_block.transpose(0, 2, 1, 3, 4).reshape(
        seq_count, kv_count, row_count, head_dim
    )
    fresh_keys = new_keys.reshape(seq_count, new_count, kv_count, head_dim).transpose(0, 2, 1, 3)
    fresh_values = new_values.reshape(seq_count, new_count, kv_count, head_dim).transpose(
        0, 2, 1, 3
    )
    cache_scores = (
        jnp.einsum("skrd,skdl->skrl", query_block, key_cache, preferred_element_type=jnp.float32)
        * scale
    )
    in_cache = jnp.arange(length)[None, :] < cache_lengths[:, None]
    cache_scores = jnp.where(in_cache[:, None, None, :], cache_scores, -1e30)
    fresh_scores = (
        jnp.einsum("skrd,sknd->skrn", query_block, fresh_keys, preferred_element_type=jnp.float32)
        * scale
    )
    causal = (jnp.arange(row_count) // group_size)[:, None] >= jnp.arange(new_count)[None, :]
    fresh_scores = jnp.where(causal[None, None, :, :], fresh_scores, -1e30)
    row_max = jnp.maximum(
        jnp.max(cache_scores, -1, keepdims=True), jnp.max(fresh_scores, -1, keepdims=True)
    )
    cache_exp = jnp.exp(cache_scores - row_max)
    fresh_exp = jnp.exp(fresh_scores - row_max)
    denom_sum = jnp.sum(cache_exp, -1, keepdims=True) + jnp.sum(fresh_exp, -1, keepdims=True)
    cache_probs = (cache_exp / denom_sum).astype(jnp.bfloat16)
    fresh_probs = (fresh_exp / denom_sum).astype(jnp.bfloat16)
    head_mix = jnp.einsum(
        "skrl,skdl->skrd", cache_probs, value_cache, preferred_element_type=jnp.float32
    )
    head_mix = head_mix + jnp.einsum(
        "skrn,sknd->skrd", fresh_probs, fresh_values, preferred_element_type=jnp.float32
    )
    head_mix = head_mix.reshape(seq_count, kv_count, new_count, group_size, head_dim).transpose(
        0, 2, 1, 3, 4
    )
    return head_mix.reshape(seq_count * new_count, kv_count * group_size * head_dim).astype(
        jnp.bfloat16
    )


def expert_apply(received, w_gate, w_up, w_down):
    width = received.shape[-1]
    flat_rows = received.reshape(-1, width)
    gate_proj = jnp.dot(flat_rows, w_gate[0], preferred_element_type=jnp.float32)
    up_proj = jnp.dot(flat_rows, w_up[0], preferred_element_type=jnp.float32)
    activated = ((up_proj + 1.0) * gate_proj * jax.nn.sigmoid(1.702 * gate_proj)).astype(
        jnp.bfloat16
    )
    partial_out = jnp.dot(activated, w_down[0], preferred_element_type=jnp.float32)
    return partial_out.reshape(received.shape[0], received.shape[1], width)


def sparse_body(
    hidden,
    queries,
    new_keys,
    new_values,
    key_cache,
    value_cache,
    cache_lengths,
    w_out,
    w_router,
    routes,
    w_gate,
    w_up,
    w_down,
):
    tp_size = lax.axis_size("tp")
    tp_index = lax.axis_index("tp")
    width = hidden.shape[1]
    block_rows = hidden.shape[0] // tp_size
    top_count = routes.shape[1]
    experts = w_router.shape[1]
    capacity = min(block_rows, max(2, (2 * block_rows * top_count + experts - 1) // experts))
    start_row = tp_index * block_rows
    attended = attend(queries, new_keys, new_values, key_cache, value_cache, cache_lengths)
    partial_value = jnp.dot(attended, w_out, preferred_element_type=jnp.float32)
    summed = lax.psum_scatter(
        partial_value.astype(jnp.bfloat16), "tp", scatter_dimension=0, tiled=True
    ).astype(jnp.float32)
    residual = (
        lax.dynamic_slice_in_dim(hidden, start_row, block_rows, 0).astype(jnp.float32) + summed
    )
    local_routes = lax.dynamic_slice_in_dim(routes, start_row, block_rows, 0)
    block_count = 1
    normed = (
        residual * lax.rsqrt(jnp.mean(residual * residual, -1, keepdims=True) + 1e-05)
    ).astype(jnp.bfloat16)
    logits = jnp.dot(normed, w_router, preferred_element_type=jnp.float32)
    expert_ids = jnp.arange(experts, dtype=jnp.int32)
    matches = local_routes[:, :, None] == expert_ids[None, None, :]
    picked = jnp.sum(jnp.where(matches, logits[:, None, :], 0.0), -1)
    picked_exp = jnp.exp(picked)
    weights = picked_exp / jnp.sum(picked_exp, -1, keepdims=True)
    flat_routes = local_routes.reshape(-1)
    one_hot = (
        flat_routes.reshape(block_count, block_rows * top_count)[:, :, None]
        == expert_ids[None, None, :]
    ).astype(jnp.int32)
    slot_rank = jnp.sum((jnp.cumsum(one_hot, 1) - one_hot) * one_hot, -1)
    slot_index = (
        slot_rank + (jnp.arange(block_count, dtype=jnp.int32) * capacity)[:, None]
    ).reshape(-1)
    outgoing = jnp.zeros((experts, block_count * capacity, width), jnp.bfloat16)
    outgoing = outgoing.at[flat_routes, slot_index].set(jnp.repeat(normed, top_count, axis=0))
    grouped = expert_apply(
        lax.all_gather(
            lax.all_to_all(outgoing, "ep", split_axis=0, concat_axis=0, tiled=True),
            "tp",
            axis=1,
            tiled=True,
        ),
        w_gate,
        w_up,
        w_down,
    )
    group_total = lax.psum_scatter(
        grouped.astype(jnp.bfloat16), "tp", scatter_dimension=1, tiled=True
    ).astype(jnp.float32)
    returned = lax.all_to_all(
        group_total.astype(jnp.bfloat16), "ep", split_axis=0, concat_axis=0, tiled=True
    ).astype(group_total.dtype)
    routed = returned[flat_routes, slot_index].reshape(-1, top_count, width)
    mixture = jnp.sum(weights[:, :, None] * routed, 1)
    return (residual + mixture).astype(jnp.bfloat16)


def swap(value, axis, step):
    size = lax.axis_size(axis)
    return lax.ppermute(value, axis, [(i, i ^ step) for i in range(size)])


def turn(value, axis, lines, step):
    size = lax.axis_size(axis)
    return lax.ppermute(value, axis, [(i, (i + step * lines) % size) for i in range(size)])


def dense_body(
    hidden,
    queries,
    new_keys,
    new_values,
    key_cache,
    value_cache,
    cache_lengths,
    w_out,
    w_router,
    routes,
    w_gate,
    w_up,
    w_down,
):
    ep_size = lax.axis_size("ep")
    tp_size = lax.axis_size("tp")
    ep_index = lax.axis_index("ep")
    tp_index = lax.axis_index("tp")
    half, side = tp_index // 2, tp_index % 2
    halves = tp_size // 2
    width = hidden.shape[1]
    block_rows = hidden.shape[0] // tp_size
    experts = w_router.shape[1]
    pad = -width % 128
    own_rows = halves * block_rows

    def pick(value, index, axis):
        return lax.dynamic_index_in_dim(value, index, axis, keepdims=False)

    attended = attend(queries, new_keys, new_values, key_cache, value_cache, cache_lengths)
    partial_value = jnp.dot(attended, w_out, preferred_element_type=jnp.float32)
    partial_value = partial_value.reshape(halves, 2, block_rows, width)
    passed = swap(pick(partial_value, 1 - side, 1).astype(jnp.bfloat16), "tp", 1)
    chip_value = pick(partial_value, side, 1) + passed.astype(jnp.float32)
    across = swap(chip_value.astype(jnp.bfloat16), "tp", 2)
    own_hidden = pick(hidden.reshape(halves, 2, block_rows, width), side, 1)
    residual = own_hidden.astype(jnp.float32) + chip_value + across.astype(jnp.float32)
    residual = residual.reshape(own_rows, width)
    normed = (
        residual * lax.rsqrt(jnp.mean(residual * residual, -1, keepdims=True) + 1e-05)
    ).astype(jnp.bfloat16)
    logits = jnp.dot(normed, w_router, preferred_element_type=jnp.float32)
    own_routes = pick(routes.reshape(halves, 2, block_rows, -1), side, 1).reshape(own_rows, -1)
    named = jnp.any(own_routes[:, :, None] == jnp.arange(experts)[None, None, :], 1)
    picked_exp = jnp.where(named, jnp.exp(logits), 0.0)
    weights = picked_exp / jnp.sum(picked_exp, -1, keepdims=True)
    weights_high = weights.astype(jnp.bfloat16)
    weights_low = (weights - weights_high.astype(jnp.float32)).astype(jnp.bfloat16)
    filler = jnp.zeros((own_rows, pad - 2 * experts), jnp.bfloat16)
    sent = jnp.concatenate([normed, weights_high, weights_low, filler], 1)

    lines = 2
    steps = ep_size // lines
    pieces = [sent] + [turn(sent, "ep", lines, k) for k in range(1, steps)]
    gathered = []
    for piece in pieces:
        gathered += [piece, swap(piece, "ep", 1)]
    mine = jnp.stack(gathered)
    theirs = swap(mine, "tp", 1)
    rows = jnp.stack([mine, theirs]).reshape(-1, width + pad)

    flat_rows = rows[:, :width]
    scores = rows[:, width:].astype(jnp.float32)
    expert_is = jnp.arange(pad) % experts == ep_index
    in_use = jnp.arange(pad) < 2 * experts
    row_weight = jnp.sum(jnp.where((expert_is & in_use)[None, :], scores, 0.0), 1, keepdims=True)
    gate_proj = jnp.dot(flat_rows, w_gate[0], preferred_element_type=jnp.float32)
    up_proj = jnp.dot(flat_rows, w_up[0], preferred_element_type=jnp.float32)
    activated = ((up_proj + 1.0) * gate_proj * jax.nn.sigmoid(1.702 * gate_proj)).astype(
        jnp.bfloat16
    )
    mixed = jnp.dot(activated, w_down[0], preferred_element_type=jnp.float32) * row_weight
    mixed = mixed.reshape(2, steps, 2, own_rows, width)
    chip_mixed = mixed[0] + swap(mixed[1].astype(jnp.bfloat16), "tp", 1).astype(jnp.float32)
    pair = [
        chip_mixed[k, 0] + swap(chip_mixed[k, 1].astype(jnp.bfloat16), "ep", 1).astype(jnp.float32)
        for k in range(steps)
    ]
    total = pair[0]
    for k in range(1, steps):
        total = total + turn(pair[k].astype(jnp.bfloat16), "ep", lines, -k).astype(jnp.float32)
    total = total.reshape(halves, block_rows, width)
    crossed = swap(pick(total, 1 - half, 0).astype(jnp.bfloat16), "tp", 2)
    mixture = pick(total, half, 0) + crossed.astype(jnp.float32)
    base = pick(residual.reshape(halves, block_rows, width), half, 0)
    return (base + mixture).astype(jnp.bfloat16)


def body(*args):
    hidden, w_router, routes = args[0], args[8], args[9]
    tp_size, ep_size = lax.axis_size("tp"), lax.axis_size("ep")
    block_rows = hidden.shape[0] // tp_size
    experts = w_router.shape[1]
    spread = max(2, -(-2 * block_rows * routes.shape[1] // experts))
    room = -hidden.shape[1] % 128 >= 2 * experts
    if spread >= block_rows and tp_size == 4 and ep_size % 2 == 0 and room:
        return dense_body(*args)
    return sparse_body(*args)


def solution(mesh):
    return jax.shard_map(
        body,
        mesh=mesh,
        in_specs=(
            P("ep", None),
            P("ep", "tp"),
            P("ep", "tp"),
            P("ep", "tp"),
            P("ep", "tp", None, None),
            P("ep", "tp", None, None),
            P("ep"),
            P("tp", None),
            P(),
            P("ep", None),
            P("ep", None, "tp"),
            P("ep", None, "tp"),
            P("ep", "tp", None),
        ),
        out_specs=P(("ep", "tp"), None),
        check_vma=False,
    )
```

```python
import jax
import jax.numpy as jnp
from jax import lax
from jax.experimental import pallas as pl
from jax.experimental.pallas import tpu as pltpu
from jax.sharding import PartitionSpec as P


def attend(queries, new_keys, new_values, key_cache, value_cache, cache_lengths):
    seq_count, kv_count, head_dim, length = key_cache.shape
    new_count = queries.shape[0] // seq_count
    group_size = queries.shape[1] // (kv_count * head_dim)
    row_count = new_count * group_size
    scale = head_dim ** (-0.5)
    query_block = queries.reshape(seq_count, new_count, kv_count, group_size, head_dim)
    query_block = query_block.transpose(0, 2, 1, 3, 4).reshape(
        seq_count, kv_count, row_count, head_dim
    )
    fresh_keys = new_keys.reshape(seq_count, new_count, kv_count, head_dim).transpose(0, 2, 1, 3)
    fresh_values = new_values.reshape(seq_count, new_count, kv_count, head_dim).transpose(
        0, 2, 1, 3
    )
    cache_scores = (
        jnp.einsum("skrd,skdl->skrl", query_block, key_cache, preferred_element_type=jnp.float32)
        * scale
    )
    in_cache = jnp.arange(length)[None, :] < cache_lengths[:, None]
    cache_scores = jnp.where(in_cache[:, None, None, :], cache_scores, -1e30)
    fresh_scores = (
        jnp.einsum("skrd,sknd->skrn", query_block, fresh_keys, preferred_element_type=jnp.float32)
        * scale
    )
    causal = (jnp.arange(row_count) // group_size)[:, None] >= jnp.arange(new_count)[None, :]
    fresh_scores = jnp.where(causal[None, None, :, :], fresh_scores, -1e30)
    row_max = jnp.maximum(
        jnp.max(cache_scores, -1, keepdims=True), jnp.max(fresh_scores, -1, keepdims=True)
    )
    cache_exp = jnp.exp(cache_scores - row_max)
    fresh_exp = jnp.exp(fresh_scores - row_max)
    denom_sum = jnp.sum(cache_exp, -1, keepdims=True) + jnp.sum(fresh_exp, -1, keepdims=True)
    cache_probs = (cache_exp / denom_sum).astype(jnp.bfloat16)
    fresh_probs = (fresh_exp / denom_sum).astype(jnp.bfloat16)
    head_mix = jnp.einsum(
        "skrl,skdl->skrd", cache_probs, value_cache, preferred_element_type=jnp.float32
    )
    head_mix = head_mix + jnp.einsum(
        "skrn,sknd->skrd", fresh_probs, fresh_values, preferred_element_type=jnp.float32
    )
    head_mix = head_mix.reshape(seq_count, kv_count, new_count, group_size, head_dim).transpose(
        0, 2, 1, 3, 4
    )
    return head_mix.reshape(seq_count * new_count, kv_count * group_size * head_dim).astype(
        jnp.bfloat16
    )


def expert_apply(received, w_gate, w_up, w_down):
    width = received.shape[-1]
    flat_rows = received.reshape(-1, width)
    gate_proj = jnp.dot(flat_rows, w_gate[0], preferred_element_type=jnp.float32)
    up_proj = jnp.dot(flat_rows, w_up[0], preferred_element_type=jnp.float32)
    activated = ((up_proj + 1.0) * gate_proj * jax.nn.sigmoid(1.702 * gate_proj)).astype(
        jnp.bfloat16
    )
    partial_out = jnp.dot(activated, w_down[0], preferred_element_type=jnp.float32)
    return partial_out.reshape(received.shape[0], received.shape[1], width)


def sparse_body(
    hidden,
    queries,
    new_keys,
    new_values,
    key_cache,
    value_cache,
    cache_lengths,
    w_out,
    w_router,
    routes,
    w_gate,
    w_up,
    w_down,
):
    tp_size = lax.axis_size("tp")
    tp_index = lax.axis_index("tp")
    width = hidden.shape[1]
    block_rows = hidden.shape[0] // tp_size
    top_count = routes.shape[1]
    experts = w_router.shape[1]
    capacity = min(block_rows, max(2, (2 * block_rows * top_count + experts - 1) // experts))
    start_row = tp_index * block_rows
    attended = attend(queries, new_keys, new_values, key_cache, value_cache, cache_lengths)
    partial_value = jnp.dot(attended, w_out, preferred_element_type=jnp.float32)
    summed = lax.psum_scatter(
        partial_value.astype(jnp.bfloat16), "tp", scatter_dimension=0, tiled=True
    ).astype(jnp.float32)
    residual = (
        lax.dynamic_slice_in_dim(hidden, start_row, block_rows, 0).astype(jnp.float32) + summed
    )
    local_routes = lax.dynamic_slice_in_dim(routes, start_row, block_rows, 0)
    block_count = 1
    normed = (
        residual * lax.rsqrt(jnp.mean(residual * residual, -1, keepdims=True) + 1e-05)
    ).astype(jnp.bfloat16)
    logits = jnp.dot(normed, w_router, preferred_element_type=jnp.float32)
    expert_ids = jnp.arange(experts, dtype=jnp.int32)
    matches = local_routes[:, :, None] == expert_ids[None, None, :]
    picked = jnp.sum(jnp.where(matches, logits[:, None, :], 0.0), -1)
    picked_exp = jnp.exp(picked)
    weights = picked_exp / jnp.sum(picked_exp, -1, keepdims=True)
    flat_routes = local_routes.reshape(-1)
    one_hot = (
        flat_routes.reshape(block_count, block_rows * top_count)[:, :, None]
        == expert_ids[None, None, :]
    ).astype(jnp.int32)
    slot_rank = jnp.sum((jnp.cumsum(one_hot, 1) - one_hot) * one_hot, -1)
    slot_index = (
        slot_rank + (jnp.arange(block_count, dtype=jnp.int32) * capacity)[:, None]
    ).reshape(-1)
    outgoing = jnp.zeros((experts, block_count * capacity, width), jnp.bfloat16)
    outgoing = outgoing.at[flat_routes, slot_index].set(jnp.repeat(normed, top_count, axis=0))
    grouped = expert_apply(
        lax.all_gather(
            lax.all_to_all(outgoing, "ep", split_axis=0, concat_axis=0, tiled=True),
            "tp",
            axis=1,
            tiled=True,
        ),
        w_gate,
        w_up,
        w_down,
    )
    group_total = lax.psum_scatter(
        grouped.astype(jnp.bfloat16), "tp", scatter_dimension=1, tiled=True
    ).astype(jnp.float32)
    returned = lax.all_to_all(
        group_total.astype(jnp.bfloat16), "ep", split_axis=0, concat_axis=0, tiled=True
    ).astype(group_total.dtype)
    routed = returned[flat_routes, slot_index].reshape(-1, top_count, width)
    mixture = jnp.sum(weights[:, :, None] * routed, 1)
    return (residual + mixture).astype(jnp.bfloat16)


def swap(value, axis, step):
    size = lax.axis_size(axis)
    return lax.ppermute(value, axis, [(i, i ^ step) for i in range(size)])


def turn(value, axis, lines, step):
    size = lax.axis_size(axis)
    return lax.ppermute(value, axis, [(i, (i + step * lines) % size) for i in range(size)])


def run(kernel, name, scalars, arrays, outs, scratch=(), far=(), room=16):
    near = [pltpu.with_memory_space_constraint(a, pltpu.VMEM) for a in arrays]
    specs = [pl.BlockSpec(memory_space=pltpu.SMEM)] * len(scalars)
    specs += [pl.BlockSpec(memory_space=pltpu.VMEM)] * len(arrays)
    specs += [pl.BlockSpec(memory_space=pltpu.HBM)] * len(far)
    far = [pltpu.with_memory_space_constraint(a, pltpu.HBM) for a in far]
    return pl.pallas_call(
        kernel,
        name=name,
        out_shape=tuple(outs),
        in_specs=specs,
        out_specs=tuple([pl.BlockSpec(memory_space=pltpu.VMEM)] * len(outs)),
        scratch_shapes=list(scratch),
        compiler_params=pltpu.CompilerParams(vmem_limit_bytes=room << 20),
    )(*scalars, *near, *far)


def near(rows, width, kind):
    return pltpu.VMEM((rows, width), kind)


def attend_kernel(
    place, lengths, queries, new_keys, new_values, key_cache, value_cache, w_out,
    kept, passed,
    keys, values, weights, scores, mixed, total, key_sem, value_sem, weight_sem,
):
    seq_count, _, head_dim, length = key_cache.shape
    tokens = queries.shape[0]
    new_count = tokens // seq_count
    heads = queries.shape[1] // head_dim
    block = kept.shape[0] // 2
    scale = head_dim ** (-0.5)
    key_copy = pltpu.make_async_copy(key_cache, keys, key_sem)
    value_copy = pltpu.make_async_copy(value_cache, values, value_sem)
    weight_copy = pltpu.make_async_copy(w_out, weights, weight_sem)
    key_copy.start()
    value_copy.start()
    weight_copy.start()
    rows = heads * new_count
    fresh_keys, fresh_values = new_keys[...], new_values[...]
    position = lax.broadcasted_iota(jnp.int32, (rows, length), 1)
    turn_of = lax.broadcasted_iota(jnp.int32, (rows, tokens), 0) % new_count
    token = lax.broadcasted_iota(jnp.int32, (rows, tokens), 1)
    last = (((1,), (1,)), ((), ()))
    query, fresh, whole = [], [], []
    for s in range(seq_count):
        start = s * new_count
        parts = [
            queries[start : start + new_count, h * head_dim : (h + 1) * head_dim]
            for h in range(heads)
        ]
        query.append(jnp.concatenate(parts, 0))
    key_copy.wait()
    for s in range(seq_count):
        scores[s] = jnp.dot(query[s], keys[s, 0], preferred_element_type=jnp.float32)
    for s in range(seq_count):
        start = s * new_count
        part = lax.dot_general(query[s], fresh_keys, last, preferred_element_type=jnp.float32)
        seen = (token >= start) & (token - start <= turn_of)
        fresh.append(jnp.where(seen, part * scale, -1e30))
    value_copy.wait()
    for s in range(seq_count):
        cached = jnp.where(position < lengths[s], scores[s] * scale, -1e30)
        top = jnp.maximum(jnp.max(cached, -1, keepdims=True), jnp.max(fresh[s], -1, keepdims=True))
        cached = jnp.exp(cached - top)
        young = jnp.exp(fresh[s] - top)
        denom = jnp.sum(cached, -1, keepdims=True) + jnp.sum(young, -1, keepdims=True)
        mix = lax.dot_general(
            cached.astype(jnp.bfloat16), values[s, 0], last, preferred_element_type=jnp.float32
        )
        mix = mix + jnp.dot(
            young.astype(jnp.bfloat16), fresh_values, preferred_element_type=jnp.float32
        )
        mix = mix / denom
        start = s * new_count
        for h in range(heads):
            mixed[start : start + new_count, h * head_dim : (h + 1) * head_dim] = mix[
                h * new_count : (h + 1) * new_count
            ]
    weight_copy.wait()
    total[...] = lax.dot_general(
        mixed[...].astype(jnp.bfloat16), weights[...], last, preferred_element_type=jnp.float32
    )
    side = place[1]
    for y in range(2):
        mine = pl.multiple_of((2 * y + side) * block, block)
        other = pl.multiple_of((2 * y + 1 - side) * block, block)
        kept[y * block : (y + 1) * block] = total[pl.ds(mine, block)]
        passed[y * block : (y + 1) * block] = total[pl.ds(other, block)].astype(jnp.bfloat16)


def norm_kernel(place, hidden, routes, kept, passed, across, w_router, sent, base, turned):
    rows, width = kept.shape
    block = rows // 2
    half, side = place[0], place[1]
    experts = w_router.shape[0]
    residual = kept[...] + passed[...].astype(jnp.float32) + across[...].astype(jnp.float32)
    turned[...] = routes[...].T
    hidden_rows, route_rows = [], []
    for y in range(2):
        mine = pl.multiple_of((2 * y + side) * block, block)
        hidden_rows.append(hidden[pl.ds(mine, block)])
        route_rows.append(turned[pl.ds(mine, block)])
    residual = residual + jnp.concatenate(hidden_rows, 0).astype(jnp.float32)
    named = jnp.concatenate(route_rows, 0)
    for y in range(2):

        @pl.when(half == y)
        def _():
            base[:, :width] = residual[y * block : (y + 1) * block]
            base[:, width:] = jnp.zeros((block, base.shape[1] - width), jnp.float32)

    power = jnp.mean(residual * residual, -1, keepdims=True)
    normed = (residual * lax.rsqrt(power + 1e-05)).astype(jnp.bfloat16)
    sent[:, :width] = normed
    logits = lax.dot_general(
        normed, w_router[...], (((1,), (1,)), ((), ())), preferred_element_type=jnp.float32
    )
    expert = lax.broadcasted_iota(jnp.int32, (rows, experts), 1)
    chosen = expert == named[:, 0:1]
    for r in range(1, named.shape[1]):
        chosen = chosen | (expert == named[:, r : r + 1])
    picked = jnp.where(chosen, jnp.exp(logits), 0.0)
    weights = picked / jnp.sum(picked, -1, keepdims=True)
    high = weights.astype(jnp.bfloat16)
    low = (weights - high.astype(jnp.float32)).astype(jnp.bfloat16)
    rest = jnp.zeros((rows, sent.shape[1] - width - 2 * experts), jnp.bfloat16)
    sent[:, width:] = jnp.concatenate([high, low, rest], 1)


def expert_kernel(*refs):
    place = refs[0]
    count = len(refs) - 6
    pieces = refs[1 : 1 + count]
    w_gate, w_up, w_down, kept, passed = refs[1 + count :]
    width, experts = w_down.shape[0], place[3]
    rows = jnp.concatenate([piece[...] for piece in pieces], 0)
    flat = rows[:, :width]
    edge = width // 128 * 128
    lane = lax.broadcasted_iota(jnp.int32, (1, rows.shape[1] - edge), 1) - (width - edge)
    used = (lane == place[2]) | (lane == experts + place[2])
    weight = jnp.sum(jnp.where(used, rows[:, edge:].astype(jnp.float32), 0.0), 1, keepdims=True)
    gate = jnp.dot(flat, w_gate[...], preferred_element_type=jnp.float32)
    up = jnp.dot(flat, w_up[...], preferred_element_type=jnp.float32)
    activated = ((up + 1.0) * gate * jax.nn.sigmoid(1.702 * gate)).astype(jnp.bfloat16)
    split = kept.shape[0]
    for start in range(0, width, 512):
        stop = min(width, start + 512)
        out = lax.dot_general(
            activated,
            w_down[start:stop],
            (((1,), (1,)), ((), ())),
            preferred_element_type=jnp.float32,
        )
        out = out * weight
        kept[:, start:stop] = out[:split].astype(kept.dtype)
        passed[:, start:stop] = out[split:].astype(passed.dtype)
    blank = jnp.zeros((split, kept.shape[1] - width), kept.dtype)
    kept[:, width:] = blank
    passed[:, width:] = blank


def add_kernel(*refs):
    total = refs[0][...].astype(jnp.float32)
    for ref in refs[1:-1]:
        total = total + ref[...].astype(jnp.float32)
    refs[-1][...] = total[:, : refs[-1].shape[1]].astype(refs[-1].dtype)


def add(name, kind, *arrays):
    return run(add_kernel, name, (), arrays, [near(*arrays[0].shape, kind)])[0]


def merge_kernel(mine, got, *outs):
    own = outs[0].shape[0]
    for n, out in enumerate(outs):
        part = slice(n * own, (n + 1) * own)
        total = mine[part].astype(jnp.float32) + got[part].astype(jnp.float32)
        out[...] = total.astype(out.dtype)


def split_kernel(place, *refs):
    kept, passed, base = refs[-2], refs[-1], refs[-3]
    block = base.shape[0]
    total = refs[0][...].astype(jnp.float32)
    for ref in refs[1:-3]:
        total = total + ref[...].astype(jnp.float32)
    for y in range(2):

        @pl.when(place[0] == y)
        def _():
            kept[...] = base[...] + total[y * block : (y + 1) * block]
            passed[...] = total[(1 - y) * block : (2 - y) * block].astype(passed.dtype)


def dense_body(
    hidden,
    queries,
    new_keys,
    new_values,
    key_cache,
    value_cache,
    cache_lengths,
    w_out,
    w_router,
    routes,
    w_gate,
    w_up,
    w_down,
):
    ep_size = lax.axis_size("ep")
    tp_size = lax.axis_size("tp")
    ep_index = lax.axis_index("ep")
    tp_index = lax.axis_index("tp")
    half, side = tp_index // 2, tp_index % 2
    tokens, width = hidden.shape
    block_rows = tokens // tp_size
    experts = w_router.shape[1]
    pad = -width % 128
    own = 2 * block_rows
    f32, bf16 = jnp.float32, jnp.bfloat16
    place = jnp.stack([half, side, ep_index, jnp.int32(experts)]).astype(jnp.int32)
    sems = [pltpu.SemaphoreType.DMA] * 3

    kept, passed = run(
        attend_kernel,
        "attend",
        (place, cache_lengths),
        (queries, new_keys, new_values),
        (near(own, width, f32), near(own, width, bf16)),
        [
            pltpu.VMEM(key_cache.shape, bf16),
            pltpu.VMEM(value_cache.shape, bf16),
            pltpu.VMEM((width, w_out.shape[0]), bf16),
            pltpu.VMEM((key_cache.shape[0], tokens, key_cache.shape[3]), f32),
            pltpu.VMEM(queries.shape, f32),
            pltpu.VMEM((tokens, width), f32),
        ]
        + sems,
        (key_cache, value_cache, w_out.T),
    )
    passed = swap(passed, "tp", 1)
    across = swap(add("chip", bf16, kept, passed), "tp", 2)
    sent, base = run(
        norm_kernel,
        "norm",
        (place,),
        (hidden, routes.T, kept, passed, across, w_router.T),
        (near(own, width + pad, bf16), near(block_rows, width + pad, f32)),
        [pltpu.VMEM(routes.shape, jnp.int32)],
    )
    lines = 2
    steps = ep_size // lines
    order = [2, 0, 1, 3] if steps == 4 else list(range(steps - 1, -1, -1))
    groups = [order[: steps // 2], order[steps // 2 :]]
    first, second = {}, {}
    for k in order:
        with jax.named_scope(f"z{k}"):
            first[k] = turn(sent, "ep", lines, k) if k else sent
    for k in order:
        with jax.named_scope(f"x{k}"):
            second[k] = swap(first[k], "ep", 1)
    sums = []
    for g, group in enumerate(groups):
        mine = [second[k] for k in group] + [first[k] for k in group]
        theirs = []
        for n, piece in enumerate(mine):
            with jax.named_scope(f"c{g}{n}"):
                theirs.append(swap(piece, "tp", 1))
        rows = len(mine) * own
        mine_out, their_out = run(
            expert_kernel,
            f"expert{g}",
            (place,),
            (*mine, *theirs, w_gate[0], w_up[0], w_down[0].T),
            [near(rows, width + pad, bf16)] * 2,
        )
        with jax.named_scope(f"d{g}"):
            got = swap(their_out, "tp", 1)
        over_shape = [near(own, width + pad, bf16)] * len(group)
        here_shape = [near(own, width + pad, f32)] * len(group)
        merged = run(merge_kernel, f"merge{g}", (), (mine_out, got), over_shape + here_shape)
        for n, k in enumerate(group):
            with jax.named_scope(f"u{k}"):
                over = swap(merged[n], "ep", 1)
            if k:
                pair = add(f"pair{k}", bf16, merged[len(group) + n], over)
                with jax.named_scope(f"v{k}"):
                    sums.append(turn(pair, "ep", lines, -k))
            else:
                sums += [merged[len(group) + n], over]
    final, crossed = run(
        split_kernel,
        "split",
        (place,),
        (*sums, base),
        (near(block_rows, width + pad, f32), near(block_rows, width + pad, bf16)),
    )
    crossed = swap(crossed, "tp", 2)
    return run(
        add_kernel,
        "finish",
        (),
        (final, crossed),
        [jax.ShapeDtypeStruct((block_rows, width), bf16)],
    )[0]


def body(*args):
    hidden, w_router, routes = args[0], args[8], args[9]
    tp_size, ep_size = lax.axis_size("tp"), lax.axis_size("ep")
    block_rows = hidden.shape[0] // tp_size
    experts = w_router.shape[1]
    spread = max(2, -(-2 * block_rows * routes.shape[1] // experts))
    room = -hidden.shape[1] % 128 >= 2 * experts
    if spread >= block_rows and tp_size == 4 and ep_size % 2 == 0 and room:
        return dense_body(*args)
    return sparse_body(*args)


def solution(mesh):
    return jax.shard_map(
        body,
        mesh=mesh,
        in_specs=(
            P("ep", None),
            P("ep", "tp"),
            P("ep", "tp"),
            P("ep", "tp"),
            P("ep", "tp", None, None),
            P("ep", "tp", None, None),
            P("ep"),
            P("tp", None),
            P(),
            P("ep", None),
            P("ep", None, "tp"),
            P("ep", None, "tp"),
            P("ep", "tp", None),
        ),
        out_specs=P(("ep", "tp"), None),
        check_vma=False,
    )
```

```python
import jax
import jax.numpy as jnp
from jax import lax
from jax.experimental import pallas as pl
from jax.experimental.pallas import tpu as pltpu
from jax.sharding import PartitionSpec as P


def attend(queries, new_keys, new_values, key_cache, value_cache, cache_lengths):
    seq_count, kv_count, head_dim, length = key_cache.shape
    new_count = queries.shape[0] // seq_count
    group_size = queries.shape[1] // (kv_count * head_dim)
    row_count = new_count * group_size
    scale = head_dim ** (-0.5)
    query_block = queries.reshape(seq_count, new_count, kv_count, group_size, head_dim)
    query_block = query_block.transpose(0, 2, 1, 3, 4).reshape(
        seq_count, kv_count, row_count, head_dim
    )
    fresh_keys = new_keys.reshape(seq_count, new_count, kv_count, head_dim).transpose(0, 2, 1, 3)
    fresh_values = new_values.reshape(seq_count, new_count, kv_count, head_dim).transpose(
        0, 2, 1, 3
    )
    cache_scores = (
        jnp.einsum("skrd,skdl->skrl", query_block, key_cache, preferred_element_type=jnp.float32)
        * scale
    )
    in_cache = jnp.arange(length)[None, :] < cache_lengths[:, None]
    cache_scores = jnp.where(in_cache[:, None, None, :], cache_scores, -1e30)
    fresh_scores = (
        jnp.einsum("skrd,sknd->skrn", query_block, fresh_keys, preferred_element_type=jnp.float32)
        * scale
    )
    causal = (jnp.arange(row_count) // group_size)[:, None] >= jnp.arange(new_count)[None, :]
    fresh_scores = jnp.where(causal[None, None, :, :], fresh_scores, -1e30)
    row_max = jnp.maximum(
        jnp.max(cache_scores, -1, keepdims=True), jnp.max(fresh_scores, -1, keepdims=True)
    )
    cache_exp = jnp.exp(cache_scores - row_max)
    fresh_exp = jnp.exp(fresh_scores - row_max)
    denom_sum = jnp.sum(cache_exp, -1, keepdims=True) + jnp.sum(fresh_exp, -1, keepdims=True)
    cache_probs = (cache_exp / denom_sum).astype(jnp.bfloat16)
    fresh_probs = (fresh_exp / denom_sum).astype(jnp.bfloat16)
    head_mix = jnp.einsum(
        "skrl,skdl->skrd", cache_probs, value_cache, preferred_element_type=jnp.float32
    )
    head_mix = head_mix + jnp.einsum(
        "skrn,sknd->skrd", fresh_probs, fresh_values, preferred_element_type=jnp.float32
    )
    head_mix = head_mix.reshape(seq_count, kv_count, new_count, group_size, head_dim).transpose(
        0, 2, 1, 3, 4
    )
    return head_mix.reshape(seq_count * new_count, kv_count * group_size * head_dim).astype(
        jnp.bfloat16
    )


def expert_apply(received, w_gate, w_up, w_down):
    width = received.shape[-1]
    flat_rows = received.reshape(-1, width)
    gate_proj = jnp.dot(flat_rows, w_gate[0], preferred_element_type=jnp.float32)
    up_proj = jnp.dot(flat_rows, w_up[0], preferred_element_type=jnp.float32)
    activated = ((up_proj + 1.0) * gate_proj * jax.nn.sigmoid(1.702 * gate_proj)).astype(
        jnp.bfloat16
    )
    partial_out = jnp.dot(activated, w_down[0], preferred_element_type=jnp.float32)
    return partial_out.reshape(received.shape[0], received.shape[1], width)


def sparse_body(
    hidden,
    queries,
    new_keys,
    new_values,
    key_cache,
    value_cache,
    cache_lengths,
    w_out,
    w_router,
    routes,
    w_gate,
    w_up,
    w_down,
):
    tp_size = lax.axis_size("tp")
    tp_index = lax.axis_index("tp")
    width = hidden.shape[1]
    block_rows = hidden.shape[0] // tp_size
    top_count = routes.shape[1]
    experts = w_router.shape[1]
    capacity = min(block_rows, max(2, (2 * block_rows * top_count + experts - 1) // experts))
    start_row = tp_index * block_rows
    attended = attend(queries, new_keys, new_values, key_cache, value_cache, cache_lengths)
    partial_value = jnp.dot(attended, w_out, preferred_element_type=jnp.float32)
    summed = lax.psum_scatter(
        partial_value.astype(jnp.bfloat16), "tp", scatter_dimension=0, tiled=True
    ).astype(jnp.float32)
    residual = (
        lax.dynamic_slice_in_dim(hidden, start_row, block_rows, 0).astype(jnp.float32) + summed
    )
    local_routes = lax.dynamic_slice_in_dim(routes, start_row, block_rows, 0)
    block_count = 1
    normed = (
        residual * lax.rsqrt(jnp.mean(residual * residual, -1, keepdims=True) + 1e-05)
    ).astype(jnp.bfloat16)
    logits = jnp.dot(normed, w_router, preferred_element_type=jnp.float32)
    expert_ids = jnp.arange(experts, dtype=jnp.int32)
    matches = local_routes[:, :, None] == expert_ids[None, None, :]
    picked = jnp.sum(jnp.where(matches, logits[:, None, :], 0.0), -1)
    picked_exp = jnp.exp(picked)
    weights = picked_exp / jnp.sum(picked_exp, -1, keepdims=True)
    flat_routes = local_routes.reshape(-1)
    one_hot = (
        flat_routes.reshape(block_count, block_rows * top_count)[:, :, None]
        == expert_ids[None, None, :]
    ).astype(jnp.int32)
    slot_rank = jnp.sum((jnp.cumsum(one_hot, 1) - one_hot) * one_hot, -1)
    slot_index = (
        slot_rank + (jnp.arange(block_count, dtype=jnp.int32) * capacity)[:, None]
    ).reshape(-1)
    outgoing = jnp.zeros((experts, block_count * capacity, width), jnp.bfloat16)
    outgoing = outgoing.at[flat_routes, slot_index].set(jnp.repeat(normed, top_count, axis=0))
    grouped = expert_apply(
        lax.all_gather(
            lax.all_to_all(outgoing, "ep", split_axis=0, concat_axis=0, tiled=True),
            "tp",
            axis=1,
            tiled=True,
        ),
        w_gate,
        w_up,
        w_down,
    )
    group_total = lax.psum_scatter(
        grouped.astype(jnp.bfloat16), "tp", scatter_dimension=1, tiled=True
    ).astype(jnp.float32)
    returned = lax.all_to_all(
        group_total.astype(jnp.bfloat16), "ep", split_axis=0, concat_axis=0, tiled=True
    ).astype(group_total.dtype)
    routed = returned[flat_routes, slot_index].reshape(-1, top_count, width)
    mixture = jnp.sum(weights[:, :, None] * routed, 1)
    return (residual + mixture).astype(jnp.bfloat16)


def hop(value, axis, step):
    size = lax.axis_size(axis)
    return lax.ppermute(value, axis, [(i, i ^ step) for i in range(size)])


def run(kernel, scalars, arrays, outs, scratch=(), far=(), room=16):
    near_arrays = [pltpu.with_memory_space_constraint(a, pltpu.VMEM) for a in arrays]
    far_arrays = [pltpu.with_memory_space_constraint(a, pltpu.HBM) for a in far]
    specs = [pl.BlockSpec(memory_space=pltpu.SMEM)] * len(scalars)
    specs += [pl.BlockSpec(memory_space=pltpu.VMEM)] * len(arrays)
    specs += [pl.BlockSpec(memory_space=pltpu.HBM)] * len(far)
    return pl.pallas_call(
        kernel,
        out_shape=tuple(outs),
        in_specs=specs,
        out_specs=tuple([pl.BlockSpec(memory_space=pltpu.VMEM)] * len(outs)),
        scratch_shapes=list(scratch),
        compiler_params=pltpu.CompilerParams(vmem_limit_bytes=room << 20),
    )(*scalars, *near_arrays, *far_arrays)


def location():
    tp_index = lax.axis_index("tp")
    return tp_index // 2, tp_index % 2


def near(rows, width, kind):
    return pltpu.VMEM((rows, width), kind)


LAST = (((1,), (1,)), ((), ()))


def attend_kernel(
    key_cache, value_cache, w_out, queries, new_keys, new_values, lengths, hidden, routes,
    w_router,
    kept, passed, hidden_out, routes_out, router_out,
    keys, values, weights, query_rows, fresh_keys, fresh_values, limits, scores, mixed, total, sems,
):
    seq_count, _, head_dim, length = key_cache.shape
    tokens = queries.shape[0]
    new_count = tokens // seq_count
    heads = queries.shape[1] // head_dim
    block = kept.shape[0] // 2
    scale = head_dim ** (-0.5)
    _, side = location()
    pairs = [
        (key_cache, keys),
        (queries, query_rows),
        (new_keys, fresh_keys),
        (lengths, limits),
        (value_cache, values),
        (new_values, fresh_values),
        (w_out, weights),
        (hidden, hidden_out),
        (routes, routes_out),
        (w_router, router_out),
    ]
    copies = [pltpu.make_async_copy(a, b, sems.at[n]) for n, (a, b) in enumerate(pairs)]
    for copy in copies:
        copy.start()
    rows = heads * new_count
    position = lax.broadcasted_iota(jnp.int32, (rows, length), 1)
    turn_of = lax.broadcasted_iota(jnp.int32, (rows, tokens), 0) % new_count
    token = lax.broadcasted_iota(jnp.int32, (rows, tokens), 1)
    query, fresh = [], []
    copies[1].wait()
    for s in range(seq_count):
        start = s * new_count
        parts = [
            query_rows[start : start + new_count, h * head_dim : (h + 1) * head_dim]
            for h in range(heads)
        ]
        query.append(jnp.concatenate(parts, 0))
    copies[2].wait()
    copies[3].wait()
    copies[0].wait()
    for s in range(seq_count):
        scores[s] = jnp.dot(query[s], keys[s, 0], preferred_element_type=jnp.float32)
    for s in range(seq_count):
        start = s * new_count
        part = lax.dot_general(query[s], fresh_keys[...], LAST, preferred_element_type=jnp.float32)
        seen = (token >= start) & (token - start <= turn_of)
        fresh.append(jnp.where(seen, part * scale, -1e30))
    copies[4].wait()
    copies[5].wait()
    for s in range(seq_count):
        cached = jnp.where(position < limits[s], scores[s] * scale, -1e30)
        top = jnp.maximum(jnp.max(cached, -1, keepdims=True), jnp.max(fresh[s], -1, keepdims=True))
        cached = jnp.exp(cached - top)
        young = jnp.exp(fresh[s] - top)
        denom = jnp.sum(cached, -1, keepdims=True) + jnp.sum(young, -1, keepdims=True)
        mix = lax.dot_general(
            cached.astype(jnp.bfloat16), values[s, 0], LAST, preferred_element_type=jnp.float32
        )
        mix = mix + jnp.dot(
            young.astype(jnp.bfloat16), fresh_values[...], preferred_element_type=jnp.float32
        )
        mix = mix / denom
        start = s * new_count
        for h in range(heads):
            mixed[start : start + new_count, h * head_dim : (h + 1) * head_dim] = mix[
                h * new_count : (h + 1) * new_count
            ]
    copies[6].wait()
    total[...] = lax.dot_general(
        mixed[...].astype(jnp.bfloat16), weights[...], LAST, preferred_element_type=jnp.float32
    )
    for y in range(2):
        mine = pl.multiple_of((2 * y + side) * block, block)
        other = pl.multiple_of((2 * y + 1 - side) * block, block)
        kept[y * block : (y + 1) * block] = total[pl.ds(mine, block)]
        passed[y * block : (y + 1) * block] = total[pl.ds(other, block)].astype(jnp.bfloat16)
    for copy in copies[7:]:
        copy.wait()


def norm_kernel(
    routes, kept, passed, across, w_router, all_hidden, sent, base, turned
):
    rows, width = kept.shape
    block = rows // 2
    half, side = location()
    experts = w_router.shape[0]
    residual = kept[...] + passed[...].astype(jnp.float32) + across[...].astype(jnp.float32)
    turned[...] = routes[...].T
    hidden_rows, route_rows = [], []
    for y in range(2):
        mine = pl.multiple_of((2 * y + side) * block, block)
        hidden_rows.append(all_hidden[pl.ds(mine, block)])
        route_rows.append(turned[pl.ds(mine, block)])
    residual = residual + jnp.concatenate(hidden_rows, 0).astype(jnp.float32)
    named = jnp.concatenate(route_rows, 0)
    for y in range(2):

        @pl.when(half == y)
        def _():
            base[:, :width] = residual[y * block : (y + 1) * block]
            base[:, width:] = jnp.zeros((block, base.shape[1] - width), jnp.float32)

    power = jnp.mean(residual * residual, -1, keepdims=True)
    normed = (residual * lax.rsqrt(power + 1e-05)).astype(jnp.bfloat16)
    sent[:, :width] = normed
    logits = lax.dot_general(normed, w_router[...], LAST, preferred_element_type=jnp.float32)
    expert = lax.broadcasted_iota(jnp.int32, (rows, experts), 1)
    chosen = expert == named[:, 0:1]
    for r in range(1, named.shape[1]):
        chosen = chosen | (expert == named[:, r : r + 1])
    picked = jnp.where(chosen, jnp.exp(logits), 0.0)
    weights = picked / jnp.sum(picked, -1, keepdims=True)
    high = weights.astype(jnp.bfloat16)
    low = (weights - high.astype(jnp.float32)).astype(jnp.bfloat16)
    rest = jnp.zeros((rows, sent.shape[1] - width - 2 * experts), jnp.bfloat16)
    sent[:, width:] = jnp.concatenate([high, low, rest], 1)


def expert_kernel(*refs):
    count = len(refs) - 5
    pieces = refs[:count]
    w_gate, w_up, w_down, kept, passed = refs[count:]
    width, experts = w_down.shape[0], lax.axis_size("ep")
    expert = lax.axis_index("ep")
    rows = jnp.concatenate([piece[...] for piece in pieces], 0)
    flat = rows[:, :width]
    edge = width // 128 * 128
    lane = lax.broadcasted_iota(jnp.int32, (1, rows.shape[1] - edge), 1) - (width - edge)
    used = (lane == expert) | (lane == experts + expert)
    weight = jnp.sum(jnp.where(used, rows[:, edge:].astype(jnp.float32), 0.0), 1, keepdims=True)
    gate = jnp.dot(flat, w_gate[...], preferred_element_type=jnp.float32)
    up = jnp.dot(flat, w_up[...], preferred_element_type=jnp.float32)
    activated = ((up + 1.0) * gate * jax.nn.sigmoid(1.702 * gate)).astype(jnp.bfloat16)
    split = kept.shape[0]
    for start in range(0, width, 512):
        stop = min(width, start + 512)
        out = lax.dot_general(
            activated, w_down[start:stop], LAST, preferred_element_type=jnp.float32
        )
        out = out * weight
        kept[:, start:stop] = out[:split].astype(kept.dtype)
        passed[:, start:stop] = out[split:].astype(passed.dtype)
    blank = jnp.zeros((split, kept.shape[1] - width), kept.dtype)
    kept[:, width:] = blank
    passed[:, width:] = blank


def add_kernel(*refs):
    total = refs[0][...].astype(jnp.float32)
    for ref in refs[1:-1]:
        total = total + ref[...].astype(jnp.float32)
    refs[-1][...] = total[:, : refs[-1].shape[1]].astype(refs[-1].dtype)


def add(kind, *arrays):
    return run(add_kernel, (), arrays, [near(*arrays[0].shape, kind)])[0]


def join_kernel(*refs):
    out, start = refs[-1], 0
    for ref in refs[:-1]:
        out[start : start + ref.shape[0]] = ref[...]
        start += ref.shape[0]


def join(*arrays):
    rows = sum(a.shape[0] for a in arrays)
    return run(join_kernel, (), arrays, [near(rows, arrays[0].shape[1], arrays[0].dtype)])[0]


def merge_kernel(mine, got, *outs):
    own = outs[0].shape[0]
    for n, out in enumerate(outs):
        part = slice(n * own, (n + 1) * own)
        total = mine[part].astype(jnp.float32) + got[part].astype(jnp.float32)
        out[...] = total.astype(out.dtype)


def halve(index, total, home, away, count):
    block = home.shape[0] // count
    for y in range(2):

        @pl.when(index == y)
        def _():
            for n in range(count):
                kept = total[(2 * n + y) * block : (2 * n + y + 1) * block]
                sent = total[(2 * n + 1 - y) * block : (2 * n + 2 - y) * block]
                home[n * block : (n + 1) * block] = kept
                away[n * block : (n + 1) * block] = sent.astype(away.dtype)


def merge_far_kernel(mine, got, home, away):
    halve(location()[0], mine[...].astype(jnp.float32) + got[...].astype(jnp.float32), home, away, 2)


def near_kernel(base, *refs):
    home, away = refs[-2:]
    total = refs[0][...].astype(jnp.float32)
    for ref in refs[1:-2]:
        total = total + ref[...].astype(jnp.float32)
    block = base.shape[0]
    for y in range(2):

        @pl.when(location()[0] == y)
        def _():
            home[...] = base[...] + total[y * block : (y + 1) * block]
            away[...] = total[(1 - y) * block : (2 - y) * block].astype(away.dtype)


def across_kernel(home, got, over, here):
    own = over.shape[0]
    rows = home[...] + got[...].astype(jnp.float32)
    over[...] = rows[:own].astype(over.dtype)
    here[...] = rows[own:]


def dense_body(
    hidden,
    queries,
    new_keys,
    new_values,
    key_cache,
    value_cache,
    cache_lengths,
    w_out,
    w_router,
    routes,
    w_gate,
    w_up,
    w_down,
):
    ep_size = lax.axis_size("ep")
    tp_size = lax.axis_size("tp")
    tokens, width = hidden.shape
    block_rows = tokens // tp_size
    experts = w_router.shape[1]
    pad = -width % 128
    own = 2 * block_rows
    f32, bf16 = jnp.float32, jnp.bfloat16

    kept, passed, all_hidden, own_routes, router = run(
        attend_kernel,
        (),
        (),
        (
            near(own, width, f32),
            near(own, width, bf16),
            near(tokens, width, bf16),
            pltpu.VMEM(routes.shape[::-1], jnp.int32),
            near(experts, width, bf16),
        ),
        [
            pltpu.VMEM(key_cache.shape, bf16),
            pltpu.VMEM(value_cache.shape, bf16),
            pltpu.VMEM((width, w_out.shape[0]), bf16),
            pltpu.VMEM(queries.shape, bf16),
            pltpu.VMEM(new_keys.shape, bf16),
            pltpu.VMEM(new_values.shape, bf16),
            pltpu.SMEM(cache_lengths.shape, jnp.int32),
            pltpu.VMEM((key_cache.shape[0], tokens, key_cache.shape[3]), f32),
            pltpu.VMEM(queries.shape, f32),
            pltpu.VMEM((tokens, width), f32),
            pltpu.SemaphoreType.DMA((10,)),
        ],
        (
            key_cache, value_cache, w_out.T, queries, new_keys, new_values, cache_lengths,
            hidden, routes.T, w_router.T,
        ),
    )
    passed = hop(passed, "tp", 1)
    across = hop(add(bf16, kept, passed), "tp", 2)
    sent, base = run(
        norm_kernel,
        (),
        (own_routes, kept, passed, across, router, all_hidden),
        (near(own, width + pad, bf16), near(block_rows, width + pad, f32)),
        [pltpu.VMEM(routes.shape, jnp.int32)],
    )
    steps = ep_size // 2
    first = {0: sent}
    for k in range(1, steps):
        low = k & -k
        if low == k:
            first[k] = hop(sent, "ep", 2 * k)
        else:
            first[k] = hop(first[k - low], "ep", 2 * low)
    tall = width + pad
    near_sums, far_sums = [], []
    for k in range(steps):
        second = hop(first[k], "ep", 1)
        mine = join(second, first[k])
        theirs = hop(mine, "tp", 1)
        mine_out, their_out = run(
            expert_kernel,
            (),
            (mine, theirs, w_gate[0], w_up[0], w_down[0].T),
            [near(2 * own, tall, bf16)] * 2,
        )
        got = hop(their_out, "tp", 1)
        if k < 2:
            over, here = run(
                merge_kernel, (), (mine_out, got), [near(own, tall, bf16), near(own, tall, f32)]
            )
        else:
            home, away = run(
                merge_far_kernel, (), (mine_out, got), [near(own, tall, f32), near(own, tall, bf16)]
            )
            over, here = run(
                across_kernel,
                (),
                (home, hop(away, "tp", 2)),
                [near(block_rows, tall, bf16), near(block_rows, tall, f32)],
            )
        over = hop(over, "ep", 1)
        sums = near_sums if k < 2 else far_sums
        if k:
            pair = add(bf16, here, over)
            sums.append(hop(pair, "ep", 2 * k))
        else:
            sums += [here, over]
    home, away = run(
        near_kernel,
        (),
        (base, *near_sums),
        [near(block_rows, tall, f32), near(block_rows, tall, bf16)],
    )
    return run(
        add_kernel,
        (),
        (home, hop(away, "tp", 2), *far_sums),
        [jax.ShapeDtypeStruct((block_rows, width), bf16)],
    )[0]


def body(*args):
    hidden, w_router, routes = args[0], args[8], args[9]
    tp_size, ep_size = lax.axis_size("tp"), lax.axis_size("ep")
    block_rows = hidden.shape[0] // tp_size
    experts = w_router.shape[1]
    spread = max(2, -(-2 * block_rows * routes.shape[1] // experts))
    room = -hidden.shape[1] % 128 >= 2 * experts
    if spread >= block_rows and tp_size == 4 and ep_size == 8 and room:
        return dense_body(*args)
    return sparse_body(*args)


def solution(mesh):
    return jax.shard_map(
        body,
        mesh=mesh,
        in_specs=(
            P("ep", None),
            P("ep", "tp"),
            P("ep", "tp"),
            P("ep", "tp"),
            P("ep", "tp", None, None),
            P("ep", "tp", None, None),
            P("ep"),
            P("tp", None),
            P(),
            P("ep", None),
            P("ep", None, "tp"),
            P("ep", None, "tp"),
            P("ep", "tp", None),
        ),
        out_specs=P(("ep", "tp"), None),
        check_vma=False,
    )
```
